512 devices in a mesh: wn: 16 (over y, core), sp: 32 (over x, z).
Axes of the slice: x: 4, y: 8, z: 8, core: 2. Of those that a mesh axis runs over, the one named last changes fastest.
Arguments:
- random_slabs: float32 [8, 3, 2048, 4096], P(None, None, 'wn', 'sp'), may hold values from -6 to 6
- stress: float32 [6, 2048], P(None, 'wn'), may hold values from -0.8 to 2, as said below
- profile: float32 [2048], P('wn'), may hold values from 0.2 to 1.2
Outputs:
- inflow: float32 [8, 3, 2048, 4096], P(None, None, 'wn', 'sp')
The draws below stay inside these ranges and needn't reach their ends.
Inputs may be any that keep to these rules, and one draw needn't show every extreme that they name: R11, R22 and R33 are positive, and each off-diagonal stress is at most 0.4 times the square root of the product of its two diagonal stresses in magnitude.
All inputs are finite; a program needn't handle non-finite values.
Results may differ from the reference program's by a relative error of at most 0.0003.
Values sent between devices are 32-bit elements; how exact they have to be, the bound alone decides.
No kernel may reach another device: no remote copies, remote signals or barrier semaphores. Data moves between devices by JAX's collectives and lax.ppermute only.
A program may use at most 128 MiB of HBM per device.

```python
import jax
import jax.numpy as jnp
from jax import lax

STEPS = 8
H = 64
NY = 2048
NZ = 4096


carry_over = 0.85


def draw_random_slabs(key, part):
    source = jax.random.truncated_normal(key, -1.7, 1.7, (STEPS, 3, NY + 1, NZ + 1), jnp.float32)
    here = source[:, :, 1:, 1:]
    below = source[:, :, :-1, 1:]
    beside = source[:, :, 1:, :-1]
    corner = source[:, :, :-1, :-1]
    return here - carry_over * below - carry_over * beside + carry_over * carry_over * corner


def draw_stress(key, part):
    diag_key = jax.random.fold_in(key, 11)
    corr_key = jax.random.fold_in(key, 23)
    diagonal = jnp.exp(jax.random.uniform(diag_key, (3, NY), jnp.float32, jnp.log(0.5), jnp.log(2.0)))
    correlation = jax.random.uniform(corr_key, (3, NY), jnp.float32, -0.4, 0.4)
    cross_yx = correlation[0] * jnp.sqrt(diagonal[0] * diagonal[1])
    cross_zx = correlation[1] * jnp.sqrt(diagonal[0] * diagonal[2])
    cross_zy = correlation[2] * jnp.sqrt(diagonal[1] * diagonal[2])
    return jnp.concatenate([diagonal, jnp.stack([cross_yx, cross_zx, cross_zy])], axis=0)


def steps_of(rng, dims, pieces, least, largest):
    def one(position, shards_of):
        steps = jax.random.uniform(jax.random.fold_in(jax.random.fold_in(rng, 6), position), (shards_of,), jnp.float32, least / len(pieces), largest / len(pieces))
        return jnp.repeat(jnp.exp(steps), dims[position] // shards_of).reshape((-1,) + (1,) * (len(dims) - position - 1))

    factor_of = one(*pieces[0])
    for cut in pieces[1:]:
        factor_of = factor_of * one(*cut)
    return factor_of


def setup_inputs(seed: int = 0) -> dict:
    splits = jax.random.split(jax.random.key(seed), 4)
    random_slabs = draw_random_slabs(jax.random.fold_in(splits[3], 71), 0)
    stress = draw_stress(jax.random.fold_in(splits[3], 71), 0)
    profile = jnp.clip(0.2 + 1 * jax.random.uniform(splits[2], (NY,), jnp.float32) ** steps_of(splits[2], (NY,), ((0, 16),), -0.2, 0.2), 0.2, 1.2)
    return dict(random_slabs=random_slabs, stress=stress, profile=profile)


def band_matrix(reach):
    width = 2 * reach
    offset = jnp.arange(-reach, reach + 1).astype(jnp.float32)
    scale_len = reach / 2.0
    norming = jnp.sqrt(jnp.sum(jnp.exp(-jnp.pi * offset * offset / (scale_len * scale_len))))
    source = jnp.arange(2 * width)[:, None]
    target = jnp.arange(width)[None, :]
    lag = (source - target - reach).astype(jnp.float32)
    values = jnp.exp(-jnp.pi * lag * lag / (2.0 * scale_len * scale_len)) / norming
    return jnp.where(jnp.abs(lag) <= reach, values, 0.0).astype(jnp.float32)

def filter_last(padded, reach):
    width = 2 * reach
    band = band_matrix(reach)
    lead = padded.shape[:-1]
    blocks = padded.reshape(lead + (padded.shape[-1] // width, width))
    upper = jnp.matmul(blocks[..., :-1, :], band[:width], precision=lax.Precision.HIGHEST)
    lower = jnp.matmul(blocks[..., 1:, :], band[width:], precision=lax.Precision.HIGHEST)
    return (upper + lower).reshape(lead + (padded.shape[-1] - width,))

def filter_rows(padded, reach):
    width = 2 * reach
    band = band_matrix(reach)
    steps_n, comps, length, cols = padded.shape
    blocks = padded.reshape(steps_n, comps, length // width, width, cols)
    upper = jnp.einsum('scbjz,ji->scbiz', blocks[:, :, :-1], band[:width], precision=lax.Precision.HIGHEST)
    lower = jnp.einsum('scbjz,ji->scbiz', blocks[:, :, 1:], band[width:], precision=lax.Precision.HIGHEST)
    return (upper + lower).reshape(steps_n, comps, length - width, cols)

def lund(scaled, stress, profile):
    chol_xx = jnp.sqrt(stress[0])
    chol_yx = stress[3] / chol_xx
    chol_yy = jnp.sqrt(stress[1] - chol_yx * chol_yx)
    chol_zx = stress[4] / chol_xx
    chol_zy = (stress[5] - chol_yx * chol_zx) / chol_yy
    chol_zz = jnp.sqrt(stress[2] - chol_zx * chol_zx - chol_zy * chol_zy)
    first = profile[:, None] + chol_xx[:, None] * scaled[:, 0]
    second = chol_yx[:, None] * scaled[:, 0] + chol_yy[:, None] * scaled[:, 1]
    third = chol_zx[:, None] * scaled[:, 0] + chol_zy[:, None] * scaled[:, 1] + chol_zz[:, None] * scaled[:, 2]
    return jnp.stack([first, second, third], axis=1)

def reference(random_slabs, stress, profile):
    padded = jnp.pad(random_slabs, ((0, 0), (0, 0), (H, H), (0, 0)))
    normal_pass = filter_rows(padded, H)
    wrapped = jnp.concatenate([normal_pass[..., -H:], normal_pass, normal_pass[..., :H]], axis=-1)
    filtered = filter_last(wrapped, H)
    row_mean = lax.optimization_barrier(jnp.sum(filtered, axis=-1)) / NZ
    centred = filtered - row_mean[..., None]
    row_var = lax.optimization_barrier(jnp.sum(centred * centred, axis=-1)) / NZ
    scaled = centred / jnp.sqrt(row_var[..., None] + 1e-06)
    return lund(scaled, stress, profile)
```

```python
import functools

import jax
import jax.numpy as jnp
import numpy as np
from jax import lax
from jax.experimental import pallas as pl
from jax.experimental.pallas import tpu as pltpu
from jax.sharding import PartitionSpec as P

H = 64
T = 128
EPS = 1e-06
NB = 12
F32 = jnp.float32
HI = lax.Precision.HIGHEST


def band():
    k = np.arange(-H, H + 1, dtype=np.float64)
    norm = np.sqrt(np.sum(np.exp(-np.pi * k * k / (H / 2.0) ** 2)))
    src = np.concatenate([np.arange(T), np.arange(-H, 0), np.arange(T, T + H)])
    lag = src[:, None] - np.arange(T)[None, :]
    val = np.exp(-np.pi * lag * lag / (2.0 * (H / 2.0) ** 2)) / norm
    return np.where(np.abs(lag) <= H, val, 0.0).astype(np.float32)


def lanes_low(shape):
    return lax.broadcasted_iota(jnp.int32, shape, len(shape) - 1) < H


def half_turn(v):
    return pltpu.roll(v, H, 1)


def edges(v):
    low = lanes_low((H, T))
    a, b = v[:H], v[H:]
    right = jnp.where(low, half_turn(a), b)
    left = jnp.where(low, a, half_turn(b))
    return right, left


def joined(hl, hr):
    low = lanes_low((H, T))
    return jnp.concatenate(
        [jnp.where(low, hl, half_turn(hr)), jnp.where(low, half_turn(hl), hr)], axis=0
    )


def dot(a, b):
    return jnp.dot(a, b, precision=HI, preferred_element_type=F32)


def pack_kernel(xb, xa, top, bottom, right, left):
    for p in range(xb.shape[0]):
        top[p] = xb[p, :H]
        bottom[p] = xb[p, H:]
    for p in range(xa.shape[0]):
        r, l = edges(xa[p])
        right[p] = r
        left[p] = l


def y_pass(bt, x, up, down):
    return dot(bt[:, :T], x) + dot(bt[:, T:], jnp.concatenate([up, down], axis=0))


def z_pass(b, x, hl, hr):
    return dot(x, b[:T]) + dot(joined(hl, hr), b[T:])


def y_first_kernel(bt, x, up, down, n, right, left):
    for p in range(x.shape[0]):
        v = y_pass(bt, x[p], up[p], down[p])
        n[p] = v
        r, l = edges(v)
        right[p] = r
        left[p] = l


def z_first_kernel(b, x, hl, hr, n, top, bottom):
    for p in range(x.shape[0]):
        v = z_pass(b, x[p], hl[p], hr[p])
        n[p] = v
        top[p] = v[:H]
        bottom[p] = v[H:]


def put_stats(acc, f, p, count):
    lane = lax.broadcasted_iota(jnp.int32, (T, T), 1)
    mean = jnp.sum(f, axis=1, keepdims=True) * (1.0 / T)
    c = f - mean
    second = jnp.sum(c * c, axis=1, keepdims=True)
    acc = jnp.where(lane == p, mean, acc)
    return jnp.where(lane == p + count, second, acc)


def z_last_kernel(b, x, hl, hr, f, st):
    count = x.shape[0]
    acc = jnp.zeros((T, T), F32)
    for p in range(count):
        v = z_pass(b, x[p], hl[p], hr[p])
        f[p] = v
        acc = put_stats(acc, v, p, count)
    st[...] = acc.T[: 2 * count]


def y_last_kernel(bt, x, up, down, f, st):
    count = x.shape[0]
    acc = jnp.zeros((T, T), F32)
    for p in range(count):
        v = y_pass(bt, x[p], up[p], down[p])
        f[p] = v
        acc = put_stats(acc, v, p, count)
    st[...] = acc.T[: 2 * count]


def final_kernel(fb, fa, sb, sa, stress, profile, out):
    steps = out.shape[0]
    s = stress[...]
    a11 = jnp.sqrt(s[0:1])
    a21 = s[3:4] / a11
    a22 = jnp.sqrt(s[1:2] - a21 * a21)
    a31 = s[4:5] / a11
    a32 = (s[5:6] - a21 * a31) / a22
    a33 = jnp.sqrt(s[2:3] - a31 * a31 - a32 * a32)
    prof = profile[...].reshape(1, T)
    done = 0
    for f, st in ((fb, sb), (fa, sa)):
        count = f.shape[0]
        parts = [st[q] for q in range(st.shape[0])]
        means = [q[:count] for q in parts]
        mean = sum(means) * (1.0 / len(parts))
        second = sum(q[count:] for q in parts)
        spread = sum((m - mean) * (m - mean) for m in means)
        per = 4096.0 / len(parts)
        var = (second + spread * per) * (1.0 / 4096.0)
        inv = 1.0 / jnp.sqrt(var + EPS)
        rows = []
        for k in range(count // 3):
            i0, i1, i2 = (inv[3 * k + c : 3 * k + c + 1] for c in range(3))
            rows += [a11 * i0, a21 * i0, a22 * i1, a31 * i0, a32 * i1, a33 * i2]
        table = jnp.concatenate(
            [mean] + rows + [prof], axis=0
        )
        pad = jnp.zeros((T - table.shape[0], T), F32)
        cols = jnp.concatenate([table, pad], axis=0).T
        pcol = cols[:, count + 2 * count : count + 2 * count + 1]
        for k in range(count // 3):
            g = [f[3 * k + c] - cols[:, 3 * k + c : 3 * k + c + 1] for c in range(3)]
            w = [cols[:, count + 6 * k + q : count + 6 * k + q + 1] for q in range(6)]
            out[done + k, 0] = pcol + w[0] * g[0]
            out[done + k, 1] = w[1] * g[0] + w[2] * g[1]
            out[done + k, 2] = w[3] * g[0] + w[4] * g[1] + w[5] * g[2]
        done += count // 3


def sds(*shape):
    return jax.ShapeDtypeStruct(shape, F32)


def planes(n, rows=T, off=0):
    return pl.BlockSpec((n, rows, T), lambda i: (i + off, 0, 0))


def whole(*shape):
    return pl.BlockSpec(shape, lambda i: (0,) * len(shape))


def shift(v, axis, d, periodic):
    n = lax.axis_size(axis)
    pairs = [(i, (i + d) % n) for i in range(n) if periodic or 0 <= i + d < n]
    return lax.ppermute(v, axis, pairs)


def groups(nx, nz):
    zs = [[x * nz + z for z in range(nz)] for x in range(nx)]
    xs = [[x * nz + z for x in range(nx)] for z in range(nz)]
    return zs, xs


def everyone(v, n, g):
    return lax.all_to_all(
        jnp.broadcast_to(v[None], (n, *v.shape)), "sp", 0, 0, axis_index_groups=g, tiled=True
    )


def merged(parts, counts, tiles):
    out, at = [], 0
    for c in counts:
        m, s = parts[:, at : at + c], parts[:, at + c : at + 2 * c]
        mean = jnp.mean(m, axis=0)
        sec = jnp.sum(s, axis=0) + tiles * T * jnp.sum((m - mean) ** 2, axis=0)
        out += [mean, sec]
        at += 2 * c
    return jnp.concatenate(out, axis=0)


def body(random_slabs, stress, profile):
    x = random_slabs.reshape(24, T, T)
    nb, na = NB, 24 - NB
    b = jnp.asarray(band())
    bt = jnp.asarray(np.ascontiguousarray(band().T))
    g = 3
    kb, ka = nb // g, na // g
    off = nb // ka
    top, bottom, right, left = pl.pallas_call(
        pack_kernel,
        grid=(g,),
        in_specs=[planes(kb), planes(ka, off=off)],
        out_specs=[planes(kb, H), planes(kb, H), planes(ka, H), planes(ka, H)],
        out_shape=[sds(nb, H, T), sds(nb, H, T), sds(na, H, T), sds(na, H, T)],
        name="pack",
    )(x, x)
    up_b = shift(bottom, "wn", 1, False)
    down_b = shift(top, "wn", -1, False)
    hl_a = shift(right, "sp", 1, True)
    hr_a = shift(left, "sp", -1, True)
    n_b, right_b, left_b = pl.pallas_call(
        y_first_kernel,
        grid=(g,),
        in_specs=[whole(T, 2 * T), planes(kb), planes(kb, H), planes(kb, H)],
        out_specs=[planes(kb), planes(kb, H), planes(kb, H)],
        out_shape=[sds(nb, T, T), sds(nb, H, T), sds(nb, H, T)],
        name="y_first",
    )(bt, x, up_b, down_b)
    hl_b = shift(right_b, "sp", 1, True)
    hr_b = shift(left_b, "sp", -1, True)
    n_a, top_a, bottom_a = pl.pallas_call(
        z_first_kernel,
        grid=(g,),
        in_specs=[whole(2 * T, T), planes(ka, off=off), planes(ka, H), planes(ka, H)],
        out_specs=[planes(ka), planes(ka, H), planes(ka, H)],
        out_shape=[sds(na, T, T), sds(na, H, T), sds(na, H, T)],
        name="z_first",
    )(b, x, hl_a, hr_a)
    up_a = shift(bottom_a, "wn", 1, False)
    down_a = shift(top_a, "wn", -1, False)
    f_b, s_b = pl.pallas_call(
        z_last_kernel,
        grid=(1,),
        in_specs=[whole(2 * T, T), planes(nb), planes(nb, H), planes(nb, H)],
        out_specs=[planes(nb), whole(2 * nb, T)],
        out_shape=[sds(nb, T, T), sds(2 * nb, T)],
        name="z_last",
    )(b, n_b, hl_b, hr_b)
    f_a, s_a = pl.pallas_call(
        y_last_kernel,
        grid=(1,),
        in_specs=[whole(T, 2 * T), planes(na), planes(na, H), planes(na, H)],
        out_specs=[planes(na), whole(2 * na, T)],
        out_shape=[sds(na, T, T), sds(2 * na, T)],
        name="y_last",
    )(bt, n_a, up_a, down_a)
    zs, xs = groups(4, 8)
    st = jnp.concatenate([s_b, s_a], axis=0)
    st = merged(everyone(st, 8, zs), (nb, na), 1)
    st = everyone(st, 4, xs)
    out = pl.pallas_call(
        final_kernel,
        out_shape=sds(8, 3, T, T),
        name="final",
    )(f_b, f_a, st[:, : 2 * nb], st[:, 2 * nb :], stress, profile)
    return out


def solution(mesh):
    return jax.shard_map(
        body,
        mesh=mesh,
        in_specs=(P(None, None, "wn", "sp"), P(None, "wn"), P("wn")),
        out_specs=P(None, None, "wn", "sp"),
        check_vma=False,
    )
```

```python
import jax
import jax.numpy as jnp
import numpy as np
from jax import lax
from jax.experimental import pallas as pl
from jax.experimental.pallas import tpu as pltpu
from jax.sharding import PartitionSpec as P


H = 64
T = 128
EPS = 1e-06
NB = 9
NA = 24 - NB
F32 = jnp.float32
BF = jnp.bfloat16


def band():
    k = np.arange(-H, H + 1, dtype=np.float64)
    norm = np.sqrt(np.sum(np.exp(-np.pi * k * k / (H / 2.0) ** 2)))
    src = np.concatenate([np.arange(T), np.arange(-H, 0), np.arange(T, T + H)])
    lag = src[:, None] - np.arange(T)[None, :]
    val = np.exp(-np.pi * lag * lag / (2.0 * (H / 2.0) ** 2)) / norm
    return np.where(np.abs(lag) <= H, val, 0.0).astype(np.float32)


def pieces(v):
    h = v.astype(BF)
    r = v - h.astype(F32)
    m = r.astype(BF)
    return h, m, (r - m.astype(F32)).astype(BF)


def bands():
    b = band()
    h = b.astype(BF)
    m = (b - h.astype(np.float32)).astype(BF)
    low = (b - h.astype(np.float32) - m.astype(np.float32)).astype(BF)
    across = np.concatenate([h, m, low], axis=1)
    return np.ascontiguousarray(across), np.ascontiguousarray(across.T)


def lanes_low(shape):
    return lax.broadcasted_iota(jnp.int32, shape, len(shape) - 1) < H


def half_turn(v):
    return pltpu.roll(v, H, 1)


def edges(v, even):
    low = lanes_low((H, T))
    a, b = v[:H], v[H:]
    right = jnp.where(low, half_turn(a), b)
    left = jnp.where(low, a, half_turn(b))
    return jnp.where(even, right, left), jnp.where(even, left, right)


def joined(re, ro, even):
    low = lanes_low((H, T))
    hl = jnp.where(even, ro, re)
    hr = jnp.where(even, re, ro)
    return jnp.concatenate(
        [jnp.where(low, hl, half_turn(hr)), jnp.where(low, half_turn(hl), hr)], axis=0
    )


def mm(a, b):
    return jnp.dot(a, b, preferred_element_type=F32)


def y_pass(bt, x, re, ro, even):
    cols = []
    for v, e, o in zip(x, re, ro):
        up = jnp.where(even, o, e)
        down = jnp.where(even, e, o)
        cols.append(jnp.concatenate([v, up, down], axis=0))
    w = cols[0] if len(cols) == 1 else jnp.concatenate(cols, axis=1)
    h, m, low = pieces(w)
    p = mm(bt, h)
    q = mm(bt[: 2 * T], m)
    r = mm(bt[:T], low)
    out = p[:T] + ((p[T : 2 * T] + q[:T]) + (p[2 * T :] + (q[T:] + r)))
    return [out[:, T * i : T * (i + 1)] for i in range(len(cols))]


def z_pass(b, x, re, ro, even):
    rows = [
        jnp.concatenate([v, joined(e, o, even)], axis=1) for v, e, o in zip(x, re, ro)
    ]
    w = rows[0] if len(rows) == 1 else jnp.concatenate(rows, axis=0)
    h, m, low = pieces(w)
    p = mm(h, b)
    q = mm(m, b[:, : 2 * T])
    r = mm(low, b[:, :T])
    out = p[:, :T] + (
        (p[:, T : 2 * T] + q[:, :T]) + (p[:, 2 * T :] + (q[:, T:] + r))
    )
    return [out[T * i : T * (i + 1)] for i in range(len(rows))]


def cuts(n, step):
    return [range(i, min(i + step, n)) for i in range(0, n, step)]


def pack_kernel(par, x, yo, ye, zo, ze):
    off = pl.multiple_of(par[1] * H, H)
    opp = pl.multiple_of(H - off, H)
    zeven = par[0] == 0
    for p in range(NB):
        yo[p] = x[p, pl.ds(off, H)]
        ye[p] = x[p, pl.ds(opp, H)]
    for p in range(NA):
        e, o = edges(x[NB + p], zeven)
        ze[p] = e
        zo[p] = o


def y_first_kernel(par, bt, x, ro, re, n, zo, ze):
    zeven, yeven = par[0] == 0, par[1] == 0
    for c in cuts(NB, 2):
        got = y_pass(bt[...], [x[p] for p in c], [re[p] for p in c], [ro[p] for p in c], yeven)
        for p, v in zip(c, got):
            n[p] = v
            e, o = edges(v, zeven)
            ze[p] = e
            zo[p] = o


def z_first_kernel(par, b, x, ro, re, n, yo, ye):
    off = par[1]
    zeven, yeven = par[0] == 0, off == 0
    for c in cuts(NA, 3):
        got = z_pass(
            b[...], [x[NB + p] for p in c], [re[p] for p in c], [ro[p] for p in c], zeven
        )
        for p, v in zip(c, got):
            n[p] = v
            yo[p] = jnp.where(yeven, v[:H], v[H:])
            ye[p] = jnp.where(yeven, v[H:], v[:H])


def put_stats(acc, f, p):
    lane = lax.broadcasted_iota(jnp.int32, (T, T), 1)
    mean = jnp.sum(f, axis=1, keepdims=True) * (1.0 / T)
    c = f - mean
    second = jnp.sum(c * c, axis=1, keepdims=True)
    acc = jnp.where(lane == p, mean, acc)
    return jnp.where(lane == p + 24, second, acc)


def z_last_kernel(par, b, x, ro, re, f, st):
    zeven = par[0] == 0
    acc = jnp.zeros((T, T), F32)
    for c in cuts(NB, 3):
        got = z_pass(b[...], [x[p] for p in c], [re[p] for p in c], [ro[p] for p in c], zeven)
        for p, v in zip(c, got):
            f[p] = v
            acc = put_stats(acc, v, p)
    st[...] = acc


def y_last_kernel(par, bt, x, ro, re, acc_b, f, st):
    yeven = par[1] == 0
    acc = acc_b[...]
    for c in cuts(NA, 2):
        got = y_pass(bt[...], [x[p] for p in c], [re[p] for p in c], [ro[p] for p in c], yeven)
        for p, v in zip(c, got):
            f[p] = v
            acc = put_stats(acc, v, p + NB)
    flat = acc.T[:48]
    for q in range(st.shape[0]):
        st[q] = flat


def merge(st, tiles):
    n = st.shape[0]
    parts = [st[q] for q in range(n)]
    mean = sum(q[:24] for q in parts) * (1.0 / n)
    second = sum(q[24:] for q in parts)
    spread = sum((q[:24] - mean) * (q[:24] - mean) for q in parts)
    return mean, second + spread * float(tiles * T)


def mid_kernel(st, out):
    mean, second = merge(st, 1)
    for q in range(out.shape[0]):
        out[q, :24] = mean
        out[q, 24:] = second


def final_kernel(fb, fa, st, stress, profile, out, buf, sems):
    mean, second = merge(st, 8)
    inv = 1.0 / jnp.sqrt(second * (1.0 / 4096.0) + EPS)
    s = stress[...]
    a11 = jnp.sqrt(s[0:1])
    a21 = s[3:4] / a11
    a22 = jnp.sqrt(s[1:2] - a21 * a21)
    a31 = s[4:5] / a11
    a32 = (s[5:6] - a21 * a31) / a22
    a33 = jnp.sqrt(s[2:3] - a31 * a31 - a32 * a32)
    prof = profile[...].reshape(1, T)
    rows = []
    for k in range(8):
        i0, i1, i2 = (inv[3 * k + c : 3 * k + c + 1] for c in range(3))
        rows += [a11 * i0, a21 * i0, a22 * i1, a31 * i0, a32 * i1, a33 * i2]
    table = jnp.concatenate([mean] + rows + [prof], axis=0)
    cols = jnp.concatenate([table, jnp.zeros((T - 73, T), F32)], axis=0).T
    pcol = cols[:, 72:73]
    copies = []
    for k in range(8):
        g = []
        for c in range(3):
            p = 3 * k + c
            v = fb[p] if p < NB else fa[p - NB]
            g.append(v - cols[:, p : p + 1])
        w = [cols[:, 24 + 6 * k + q : 25 + 6 * k + q] for q in range(6)]
        buf[k, 0] = pcol + w[0] * g[0]
        buf[k, 1] = w[1] * g[0] + w[2] * g[1]
        buf[k, 2] = w[3] * g[0] + w[4] * g[1] + w[5] * g[2]
        copy = pltpu.make_async_copy(buf.at[k], out.at[k], sems.at[k])
        copy.start()
        copies.append(copy)
    for copy in copies:
        copy.wait()


def call(kernel, ins, outs, scratch=(), hbm_out=False):
    smem = pl.BlockSpec(memory_space=pltpu.SMEM)
    vmem = pl.BlockSpec(memory_space=pltpu.VMEM)
    args, specs = [], []
    for a in ins:
        if a.dtype == jnp.int32:
            args.append(a)
            specs.append(smem)
        else:
            args.append(pltpu.with_memory_space_constraint(a, pltpu.VMEM))
            specs.append(vmem)
    if hbm_out:
        shapes = [jax.ShapeDtypeStruct(s, F32) for s in outs]
        out_specs = [pl.BlockSpec(memory_space=pl.ANY) for s in outs]
    else:
        shapes = [pltpu.VMEM(s, F32) for s in outs]
        out_specs = [vmem for s in outs]
    return pl.pallas_call(
        kernel,
        in_specs=specs,
        out_specs=out_specs,
        out_shape=shapes,
        scratch_shapes=list(scratch),
        compiler_params=pltpu.CompilerParams(vmem_limit_bytes=24 << 20),
    )(*args)


def swap(v, axis, odd, periodic):
    n = lax.axis_size(axis)
    pairs = []
    for i in range(odd, n, 2):
        j = (i + 1) % n
        if periodic or j > i:
            pairs += [(i, j), (j, i)]
    return lax.ppermute(v, axis, pairs)


def groups(nx, nz):
    zs = [[x * nz + z for z in range(nz)] for x in range(nx)]
    xs = [[x * nz + z for x in range(nx)] for z in range(nz)]
    return zs, xs


def run(random_slabs, stress, profile):
    x = random_slabs.reshape(24, T, T)
    par = jnp.stack([lax.axis_index("sp") % 2, lax.axis_index("wn") % 2]).astype(jnp.int32)
    b, bt = (jnp.asarray(v) for v in bands())
    hb, ha = (NB, H, T), (NA, H, T)
    fb, fa = (NB, T, T), (NA, T, T)
    yo, ye, zo, ze = call(pack_kernel, [par, x], [hb, hb, ha, ha])
    yo = swap(yo, "wn", 1, False)
    ye = swap(ye, "wn", 0, False)
    zo = swap(zo, "sp", 1, True)
    ze = swap(ze, "sp", 0, True)
    n_b, zo_b, ze_b = call(y_first_kernel, [par, bt, x, yo, ye], [fb, hb, hb])
    zo_b = swap(zo_b, "sp", 1, True)
    ze_b = swap(ze_b, "sp", 0, True)
    n_a, yo_a, ye_a = call(z_first_kernel, [par, b, x, zo, ze], [fa, ha, ha])
    yo_a = swap(yo_a, "wn", 1, False)
    ye_a = swap(ye_a, "wn", 0, False)
    f_b, s_b = call(z_last_kernel, [par, b, n_b, zo_b, ze_b], [fb, (T, T)])
    zs, xs = groups(4, 8)
    f_a, st = call(y_last_kernel, [par, bt, n_a, yo_a, ye_a, s_b], [fa, (8, 48, T)])
    st = lax.all_to_all(st, "sp", 0, 0, axis_index_groups=zs, tiled=True)
    (st,) = call(mid_kernel, [st], [(4, 48, T)])
    st = lax.all_to_all(st, "sp", 0, 0, axis_index_groups=xs, tiled=True)
    (out,) = call(
        final_kernel,
        [f_b, f_a, st, stress, profile],
        [(8, 3, T, T)],
        scratch=[pltpu.VMEM((8, 3, T, T), F32), pltpu.SemaphoreType.DMA((8,))],
        hbm_out=True,
    )
    return out


def solution(mesh):
    return jax.shard_map(
        run,
        mesh=mesh,
        in_specs=(P(None, None, "wn", "sp"), P(None, "wn"), P("wn")),
        out_specs=P(None, None, "wn", "sp"),
        check_vma=False,
    )
```

```python
import functools

import jax
import jax.numpy as jnp
import numpy as np
from jax import lax
from jax.experimental import pallas as pl
from jax.experimental.pallas import tpu as pltpu
from jax.sharding import PartitionSpec as P


H = 64
T = 128
EPS = 1e-06
NB = 15
NA = 24 - NB
CHUNKS = [range(i, i + 6) for i in range(0, 24, 6)]
F32 = jnp.float32
BF = jnp.bfloat16


def band():
    k = np.arange(-H, H + 1, dtype=np.float64)
    norm = np.sqrt(np.sum(np.exp(-np.pi * k * k / (H / 2.0) ** 2)))
    src = np.concatenate([np.arange(T), np.arange(-H, 0), np.arange(T, T + H)])
    lag = src[:, None] - np.arange(T)[None, :]
    val = np.exp(-np.pi * lag * lag / (2.0 * (H / 2.0) ** 2)) / norm
    return np.where(np.abs(lag) <= H, val, 0.0).astype(np.float32)


def pieces(v):
    h = v.astype(BF)
    r = v - h.astype(F32)
    m = r.astype(BF)
    return h, m, (r - m.astype(F32)).astype(BF)


def bands():
    b = band()
    h = b.astype(BF)
    m = (b - h.astype(np.float32)).astype(BF)
    low = (b - h.astype(np.float32) - m.astype(np.float32)).astype(BF)
    across = np.concatenate([h, m, low], axis=1)
    return np.ascontiguousarray(across), np.ascontiguousarray(across.T)


def lanes_low(shape):
    return lax.broadcasted_iota(jnp.int32, shape, len(shape) - 1) < H


def half_turn(v):
    return pltpu.roll(v, H, 1)


def edges(v, even):
    low = lanes_low((H, T))
    a, b = v[:H], v[H:]
    right = jnp.where(low, half_turn(a), b)
    left = jnp.where(low, a, half_turn(b))
    return jnp.where(even, right, left), jnp.where(even, left, right)


def joined(re, ro, even):
    low = lanes_low((H, T))
    hl = jnp.where(even, ro, re)
    hr = jnp.where(even, re, ro)
    return jnp.concatenate(
        [jnp.where(low, hl, half_turn(hr)), jnp.where(low, half_turn(hl), hr)], axis=0
    )


def mm(a, b):
    return jnp.dot(a, b, preferred_element_type=F32)


def y_pass(bt, x, re, ro, even):
    cols = []
    for v, e, o in zip(x, re, ro):
        up = jnp.where(even, o, e)
        down = jnp.where(even, e, o)
        cols.append(jnp.concatenate([v, up, down], axis=0))
    w = cols[0] if len(cols) == 1 else jnp.concatenate(cols, axis=1)
    h, m, low = pieces(w)
    p = mm(bt, h)
    q = mm(bt[: 2 * T], m)
    r = mm(bt[:T], low)
    out = p[:T] + ((p[T : 2 * T] + q[:T]) + (p[2 * T :] + (q[T:] + r)))
    return [out[:, T * i : T * (i + 1)] for i in range(len(cols))]


def z_pass(b, x, re, ro, even):
    rows = [
        jnp.concatenate([v, joined(e, o, even)], axis=1) for v, e, o in zip(x, re, ro)
    ]
    w = rows[0] if len(rows) == 1 else jnp.concatenate(rows, axis=0)
    h, m, low = pieces(w)
    p = mm(h, b)
    q = mm(m, b[:, : 2 * T])
    r = mm(low, b[:, :T])
    out = p[:, :T] + (
        (p[:, T : 2 * T] + q[:, :T]) + (p[:, 2 * T :] + (q[:, T:] + r))
    )
    return [out[T * i : T * (i + 1)] for i in range(len(rows))]


def cuts(n, step):
    return [range(i, min(i + step, n)) for i in range(0, n, step)]


def pack_kernel(par, src, x, yo, ye, zo, ze, sems):
    off = pl.multiple_of(par[1] * H, H)
    opp = pl.multiple_of(H - off, H)
    zeven = par[0] == 0
    copies = [
        pltpu.make_async_copy(src.at[pl.ds(c[0], len(c))], x.at[pl.ds(c[0], len(c))], sems.at[i])
        for i, c in enumerate(CHUNKS)
    ]
    for copy in copies:
        copy.start()
    for copy, c in zip(copies, CHUNKS):
        copy.wait()
        for p in c:
            if p < NB:
                yo[p] = x[p, pl.ds(off, H)]
                ye[p] = x[p, pl.ds(opp, H)]
            else:
                e, o = edges(x[p], zeven)
                ze[p - NB] = e
                zo[p - NB] = o


def y_first_kernel(par, bt, x, ro, re, n, zo, ze):
    zeven, yeven = par[0] == 0, par[1] == 0
    for c in cuts(NB, 2):
        got = y_pass(bt[...], [x[p] for p in c], [re[p] for p in c], [ro[p] for p in c], yeven)
        for p, v in zip(c, got):
            n[p] = v
            e, o = edges(v, zeven)
            ze[p] = e
            zo[p] = o


def z_first_kernel(par, b, x, ro, re, n, yo, ye):
    off = par[1]
    zeven, yeven = par[0] == 0, off == 0
    for c in cuts(NA, 3):
        got = z_pass(
            b[...], [x[NB + p] for p in c], [re[p] for p in c], [ro[p] for p in c], zeven
        )
        for p, v in zip(c, got):
            n[p] = v
            yo[p] = jnp.where(yeven, v[:H], v[H:])
            ye[p] = jnp.where(yeven, v[H:], v[:H])


def put_stats(acc, f, p):
    lane = lax.broadcasted_iota(jnp.int32, (T, T), 1)
    mean = jnp.sum(f, axis=1, keepdims=True) * (1.0 / T)
    c = f - mean
    second = jnp.sum(c * c, axis=1, keepdims=True)
    acc = jnp.where(lane == p, mean, acc)
    return jnp.where(lane == p + 24, second, acc)


def last(one_pass, step, flag, base, first, *refs):
    par, b, x, ro, re = refs[:5]
    f, st = refs[-2:]
    even = par[flag] == 0
    acc = jnp.zeros((T, T), F32) if first else refs[5][...]
    for c in cuts(f.shape[0], step):
        got = one_pass(b[...], [x[p] for p in c], [re[p] for p in c], [ro[p] for p in c], even)
        for p, v in zip(c, got):
            f[p] = v
            acc = put_stats(acc, v, base + p)
    if first:
        st[...] = acc
    else:
        flat = acc.T[:48]
        for q in range(st.shape[0]):
            st[q] = flat


def merge(st, tiles):
    n = st.shape[0]
    parts = [st[q] for q in range(n)]
    mean = sum(q[:24] for q in parts) * (1.0 / n)
    second = sum(q[24:] for q in parts)
    spread = sum((q[:24] - mean) * (q[:24] - mean) for q in parts)
    return mean, second + spread * float(tiles * T)


def mid_kernel(st, out):
    mean, second = merge(st, 1)
    for q in range(out.shape[0]):
        out[q, :24] = mean
        out[q, 24:] = second


def final_kernel(fb, fa, st, stress, profile, out, buf, sems):
    mean, second = merge(st, 8)
    inv = 1.0 / jnp.sqrt(second * (1.0 / 4096.0) + EPS)
    s = stress[...]
    a11 = jnp.sqrt(s[0:1])
    a21 = s[3:4] / a11
    a22 = jnp.sqrt(s[1:2] - a21 * a21)
    a31 = s[4:5] / a11
    a32 = (s[5:6] - a21 * a31) / a22
    a33 = jnp.sqrt(s[2:3] - a31 * a31 - a32 * a32)
    prof = profile[...].reshape(1, T)
    rows = []
    for k in range(8):
        i0, i1, i2 = (inv[3 * k + c : 3 * k + c + 1] for c in range(3))
        rows += [a11 * i0, a21 * i0, a22 * i1, a31 * i0, a32 * i1, a33 * i2]
    table = jnp.concatenate([mean] + rows + [prof], axis=0)
    cols = jnp.concatenate([table, jnp.zeros((T - 73, T), F32)], axis=0).T
    pcol = cols[:, 72:73]
    copies = []
    for k in range(8):
        g = []
        for c in range(3):
            p = 3 * k + c
            v = fb[p] if p < NB else fa[p - NB]
            g.append(v - cols[:, p : p + 1])
        w = [cols[:, 24 + 6 * k + q : 25 + 6 * k + q] for q in range(6)]
        buf[k, 0] = pcol + w[0] * g[0]
        buf[k, 1] = w[1] * g[0] + w[2] * g[1]
        buf[k, 2] = w[3] * g[0] + w[4] * g[1] + w[5] * g[2]
        copy = pltpu.make_async_copy(buf.at[k], out.at[k], sems.at[k])
        copy.start()
        copies.append(copy)
    for copy in copies:
        copy.wait()


def call(kernel, ins, outs, scratch=(), hbm_out=False, hbm_in=()):
    smem = pl.BlockSpec(memory_space=pltpu.SMEM)
    vmem = pl.BlockSpec(memory_space=pltpu.VMEM)
    args, specs = [], []
    for i, a in enumerate(ins):
        if i in hbm_in:
            args.append(pltpu.with_memory_space_constraint(a, pltpu.HBM))
            specs.append(pl.BlockSpec(memory_space=pl.ANY))
        elif a.dtype == jnp.int32:
            args.append(a)
            specs.append(smem)
        else:
            args.append(pltpu.with_memory_space_constraint(a, pltpu.VMEM))
            specs.append(vmem)
    if hbm_out:
        shapes = [jax.ShapeDtypeStruct(s, F32) for s in outs]
        out_specs = [pl.BlockSpec(memory_space=pl.ANY) for s in outs]
    else:
        shapes = [pltpu.VMEM(s, F32) for s in outs]
        out_specs = [vmem for s in outs]
    return pl.pallas_call(
        kernel,
        in_specs=specs,
        out_specs=out_specs,
        out_shape=shapes,
        scratch_shapes=list(scratch),
        compiler_params=pltpu.CompilerParams(vmem_limit_bytes=24 << 20),
    )(*args)


def swap(v, axis, odd, periodic):
    n = lax.axis_size(axis)
    pairs = []
    for i in range(odd, n, 2):
        j = (i + 1) % n
        if periodic or j > i:
            pairs += [(i, j), (j, i)]
    return lax.ppermute(v, axis, pairs)


def groups(nx, nz):
    zs = [[x * nz + z for z in range(nz)] for x in range(nx)]
    xs = [[x * nz + z for x in range(nx)] for z in range(nz)]
    return zs, xs


def run(random_slabs, stress, profile):
    x = random_slabs.reshape(24, T, T)
    par = jnp.stack([lax.axis_index("sp") % 2, lax.axis_index("wn") % 2]).astype(jnp.int32)
    b, bt = (jnp.asarray(v) for v in bands())
    hb, ha = (NB, H, T), (NA, H, T)
    fb, fa = (NB, T, T), (NA, T, T)
    x, yo, ye, zo, ze = call(
        pack_kernel,
        [par, x],
        [(24, T, T), hb, hb, ha, ha],
        scratch=[pltpu.SemaphoreType.DMA((len(CHUNKS),))],
        hbm_in=(1,),
    )
    yo = swap(yo, "wn", 1, False)
    ye = swap(ye, "wn", 0, False)
    zo = swap(zo, "sp", 1, True)
    ze = swap(ze, "sp", 0, True)
    n_b, zo_b, ze_b = call(y_first_kernel, [par, bt, x, yo, ye], [fb, hb, hb])
    zo_b = swap(zo_b, "sp", 1, True)
    ze_b = swap(ze_b, "sp", 0, True)
    n_a, yo_a, ye_a = call(z_first_kernel, [par, b, x, zo, ze], [fa, ha, ha])
    yo_a = swap(yo_a, "wn", 1, False)
    ye_a = swap(ye_a, "wn", 0, False)
    f_a, s_a = call(
        functools.partial(last, y_pass, 2, 1, NB, True), [par, bt, n_a, yo_a, ye_a], [fa, (T, T)]
    )
    f_b, st = call(
        functools.partial(last, z_pass, 3, 0, 0, False),
        [par, b, n_b, zo_b, ze_b, s_a],
        [fb, (8, 48, T)],
    )
    zs, xs = groups(4, 8)
    st = lax.all_to_all(st, "sp", 0, 0, axis_index_groups=zs, tiled=True)
    (st,) = call(mid_kernel, [st], [(4, 48, T)])
    st = lax.all_to_all(st, "sp", 0, 0, axis_index_groups=xs, tiled=True)
    (out,) = call(
        final_kernel,
        [f_b, f_a, st, stress, profile],
        [(8, 3, T, T)],
        scratch=[pltpu.VMEM((8, 3, T, T), F32), pltpu.SemaphoreType.DMA((8,))],
        hbm_out=True,
    )
    return out


def solution(mesh):
    return jax.shard_map(
        run,
        mesh=mesh,
        in_specs=(P(None, None, "wn", "sp"), P(None, "wn"), P("wn")),
        out_specs=P(None, None, "wn", "sp"),
        check_vma=False,
    )
```

```python
import functools

import jax
import jax.numpy as jnp
import numpy as np
from jax import lax
from jax.experimental import pallas as pl
from jax.experimental.pallas import tpu as pltpu
from jax.sharding import PartitionSpec as P


H = 64
T = 128
EPS = 1e-06
NB = 15
NA = 24 - NB
F32 = jnp.float32
BF = jnp.bfloat16


def band():
    k = np.arange(-H, H + 1, dtype=np.float64)
    norm = np.sqrt(np.sum(np.exp(-np.pi * k * k / (H / 2.0) ** 2)))
    src = np.concatenate([np.arange(T), np.arange(-H, 0), np.arange(T, T + H)])
    lag = src[:, None] - np.arange(T)[None, :]
    val = np.exp(-np.pi * lag * lag / (2.0 * (H / 2.0) ** 2)) / norm
    return np.where(np.abs(lag) <= H, val, 0.0).astype(np.float32)


def pieces(v):
    h = v.astype(BF)
    r = v - h.astype(F32)
    m = r.astype(BF)
    return h, m, (r - m.astype(F32)).astype(BF)


def bands():
    b = band()
    h = b.astype(BF)
    m = (b - h.astype(np.float32)).astype(BF)
    low = (b - h.astype(np.float32) - m.astype(np.float32)).astype(BF)
    across = np.concatenate([h, m, low], axis=1)
    return np.ascontiguousarray(across), np.ascontiguousarray(across.T)


def parity(axis):
    return lax.axis_index(axis) % 2


def lanes_low(shape):
    return lax.broadcasted_iota(jnp.int32, shape, len(shape) - 1) < H


def half_turn(v):
    return pltpu.roll(v, H, 1)


def edges(v, even):
    low = lanes_low((H, T))
    a, b = v[:H], v[H:]
    right = jnp.where(low, half_turn(a), b)
    left = jnp.where(low, a, half_turn(b))
    return jnp.where(even, right, left), jnp.where(even, left, right)


def joined(re, ro, even):
    low = lanes_low((H, T))
    hl = jnp.where(even, ro, re)
    hr = jnp.where(even, re, ro)
    return jnp.concatenate(
        [jnp.where(low, hl, half_turn(hr)), jnp.where(low, half_turn(hl), hr)], axis=0
    )


def mm(a, b):
    return jnp.dot(a, b, preferred_element_type=F32)


def y_pass(bt, x, re, ro, even):
    cols = []
    for v, e, o in zip(x, re, ro):
        up = jnp.where(even, o, e)
        down = jnp.where(even, e, o)
        cols.append(jnp.concatenate([v, up, down], axis=0))
    w = cols[0] if len(cols) == 1 else jnp.concatenate(cols, axis=1)
    h, m, low = pieces(w)
    p = mm(bt, h)
    q = mm(bt[: 2 * T], m)
    r = mm(bt[:T], low)
    out = p[:T] + ((p[T : 2 * T] + q[:T]) + (p[2 * T :] + (q[T:] + r)))
    return [out[:, T * i : T * (i + 1)] for i in range(len(cols))]


def z_pass(b, x, re, ro, even):
    rows = [
        jnp.concatenate([v, joined(e, o, even)], axis=1) for v, e, o in zip(x, re, ro)
    ]
    w = rows[0] if len(rows) == 1 else jnp.concatenate(rows, axis=0)
    h, m, low = pieces(w)
    p = mm(h, b)
    q = mm(m, b[:, : 2 * T])
    r = mm(low, b[:, :T])
    out = p[:, :T] + (
        (p[:, T : 2 * T] + q[:, :T]) + (p[:, 2 * T :] + (q[:, T:] + r))
    )
    return [out[T * i : T * (i + 1)] for i in range(len(rows))]


def cuts(n, step):
    return [range(i, min(i + step, n)) for i in range(0, n, step)]


def pack_y_kernel(src, yo, ye, sems):
    off = pl.multiple_of(parity("wn") * H, H)
    opp = pl.multiple_of(H - off, H)
    one = pltpu.make_async_copy(src.at[pl.ds(0, NB), pl.ds(off, H)], yo, sems.at[0])
    two = pltpu.make_async_copy(src.at[pl.ds(0, NB), pl.ds(opp, H)], ye, sems.at[1])
    one.start()
    two.start()
    one.wait()
    two.wait()


def pack_z_kernel(x, zo, ze):
    zeven = parity("sp") == 0
    for p in range(NA):
        e, o = edges(x[NB + p], zeven)
        ze[p] = e
        zo[p] = o


def y_first_kernel(bt, x, ro, re, n, zo, ze):
    zeven, yeven = parity("sp") == 0, parity("wn") == 0
    for c in cuts(NB, 2):
        got = y_pass(bt[...], [x[p] for p in c], [re[p] for p in c], [ro[p] for p in c], yeven)
        for p, v in zip(c, got):
            n[p] = v
            e, o = edges(v, zeven)
            ze[p] = e
            zo[p] = o


def z_first_kernel(b, x, ro, re, n, yo, ye):
    zeven, yeven = parity("sp") == 0, parity("wn") == 0
    for c in cuts(NA, 3):
        got = z_pass(
            b[...], [x[NB + p] for p in c], [re[p] for p in c], [ro[p] for p in c], zeven
        )
        for p, v in zip(c, got):
            n[p] = v
            yo[p] = jnp.where(yeven, v[:H], v[H:])
            ye[p] = jnp.where(yeven, v[H:], v[:H])


def put_stats(acc, f, p):
    lane = lax.broadcasted_iota(jnp.int32, (T, T), 1)
    mean = jnp.sum(f, axis=1, keepdims=True) * (1.0 / T)
    c = f - mean
    second = jnp.sum(c * c, axis=1, keepdims=True)
    acc = jnp.where(lane == p, mean, acc)
    return jnp.where(lane == p + 24, second, acc)


def last(one_pass, step, axis, base, first, *refs):
    b, x, ro, re = refs[:4]
    f, st = refs[-2:]
    even = parity(axis) == 0
    acc = jnp.zeros((T, T), F32) if first else refs[4][...]
    for c in cuts(f.shape[0], step):
        got = one_pass(b[...], [x[p] for p in c], [re[p] for p in c], [ro[p] for p in c], even)
        for p, v in zip(c, got):
            f[p] = v
            acc = put_stats(acc, v, base + p)
    if first:
        st[...] = acc
    else:
        flat = acc.T[:48]
        for q in range(st.shape[0]):
            st[q] = flat


def merge(st, tiles):
    n = st.shape[0]
    parts = [st[q] for q in range(n)]
    mean = sum(q[:24] for q in parts) * (1.0 / n)
    second = sum(q[24:] for q in parts)
    spread = sum((q[:24] - mean) * (q[:24] - mean) for q in parts)
    return mean, second + spread * float(tiles * T)


def mid_kernel(st, out):
    mean, second = merge(st, 1)
    for q in range(out.shape[0]):
        out[q, :24] = mean
        out[q, 24:] = second


def factor_kernel(stress, profile, wide):
    s = stress[...]
    a11 = jnp.sqrt(s[0:1])
    a21 = s[3:4] / a11
    a22 = jnp.sqrt(s[1:2] - a21 * a21)
    a31 = s[4:5] / a11
    a32 = (s[5:6] - a21 * a31) / a22
    a33 = jnp.sqrt(s[2:3] - a31 * a31 - a32 * a32)
    rows = [a11, a21, a22, a31, a32, a33, profile[...].reshape(1, T), a11]
    cols = jnp.concatenate(rows + [jnp.zeros((T - 8, T), F32)], axis=0).T
    for q in range(7):
        wide[q] = jnp.broadcast_to(cols[:, q : q + 1], (T, T))


def final_kernel(fb, fa, st, wide, out, buf, sems):
    mean, second = merge(st, 8)
    inv = 1.0 / jnp.sqrt(second * (1.0 / 4096.0) + EPS)
    cols = jnp.concatenate([mean, inv, jnp.zeros((T - 48, T), F32)], axis=0).T
    copies = []
    for k in range(8):
        g = []
        for c in range(3):
            p = 3 * k + c
            v = fb[p] if p < NB else fa[p - NB]
            g.append((v - cols[:, p : p + 1]) * cols[:, 24 + p : 25 + p])
        buf[k, 0] = wide[6] + wide[0] * g[0]
        buf[k, 1] = wide[1] * g[0] + wide[2] * g[1]
        buf[k, 2] = wide[3] * g[0] + wide[4] * g[1] + wide[5] * g[2]
        copy = pltpu.make_async_copy(buf.at[k], out.at[k], sems.at[k])
        copy.start()
        copies.append(copy)
    for copy in copies:
        copy.wait()


def call(kernel, ins, outs, scratch=(), hbm_out=False, hbm_in=()):
    vmem = pl.BlockSpec(memory_space=pltpu.VMEM)
    args, specs = [], []
    for i, a in enumerate(ins):
        if i in hbm_in:
            args.append(pltpu.with_memory_space_constraint(a, pltpu.HBM))
            specs.append(pl.BlockSpec(memory_space=pl.ANY))
        else:
            args.append(pltpu.with_memory_space_constraint(a, pltpu.VMEM))
            specs.append(vmem)
    if hbm_out:
        shapes = [jax.ShapeDtypeStruct(s, F32) for s in outs]
        out_specs = [pl.BlockSpec(memory_space=pl.ANY) for s in outs]
    else:
        shapes = [pltpu.VMEM(s, F32) for s in outs]
        out_specs = [vmem for s in outs]
    return pl.pallas_call(
        kernel,
        in_specs=specs,
        out_specs=out_specs,
        out_shape=shapes,
        scratch_shapes=list(scratch),
        compiler_params=pltpu.CompilerParams(vmem_limit_bytes=24 << 20),
    )(*args)


def swap(v, axis, odd, periodic):
    n = lax.axis_size(axis)
    pairs = []
    for i in range(odd, n, 2):
        j = (i + 1) % n
        if periodic or j > i:
            pairs += [(i, j), (j, i)]
    return lax.ppermute(v, axis, pairs)


def groups(nx, nz):
    zs = [[x * nz + z for z in range(nz)] for x in range(nx)]
    xs = [[x * nz + z for x in range(nx)] for z in range(nz)]
    return zs, xs


def run(random_slabs, stress, profile):
    x = random_slabs.reshape(24, T, T)
    b, bt = (jnp.asarray(v) for v in bands())
    hb, ha = (NB, H, T), (NA, H, T)
    fb, fa = (NB, T, T), (NA, T, T)
    yo, ye = call(
        pack_y_kernel,
        [x],
        [hb, hb],
        scratch=[pltpu.SemaphoreType.DMA((2,))],
        hbm_in=(0,),
    )
    yo = swap(yo, "wn", 1, False)
    zo, ze = call(pack_z_kernel, [x], [ha, ha])
    zo = swap(zo, "sp", 1, True)
    ye = swap(ye, "wn", 0, False)
    ze = swap(ze, "sp", 0, True)
    n_b, zo_b, ze_b = call(y_first_kernel, [bt, x, yo, ye], [fb, hb, hb])
    zo_b = swap(zo_b, "sp", 1, True)
    ze_b = swap(ze_b, "sp", 0, True)
    n_a, yo_a, ye_a = call(z_first_kernel, [b, x, zo, ze], [fa, ha, ha])
    yo_a = swap(yo_a, "wn", 1, False)
    ye_a = swap(ye_a, "wn", 0, False)
    (wide,) = call(factor_kernel, [stress, profile], [(7, T, T)])
    f_a, s_a = call(
        functools.partial(last, y_pass, 2, "wn", NB, True),
        [bt, n_a, yo_a, ye_a],
        [fa, (T, T)],
    )
    f_b, st = call(
        functools.partial(last, z_pass, 3, "sp", 0, False),
        [b, n_b, zo_b, ze_b, s_a],
        [fb, (8, 48, T)],
    )
    zs, xs = groups(4, 8)
    st = lax.all_to_all(st, "sp", 0, 0, axis_index_groups=zs, tiled=True)
    (st,) = call(mid_kernel, [st], [(4, 48, T)])
    st = lax.all_to_all(st, "sp", 0, 0, axis_index_groups=xs, tiled=True)
    (out,) = call(
        final_kernel,
        [f_b, f_a, st, wide],
        [(8, 3, T, T)],
        scratch=[pltpu.VMEM((8, 3, T, T), F32), pltpu.SemaphoreType.DMA((8,))],
        hbm_out=True,
    )
    return out


def solution(mesh):
    return jax.shard_map(
        run,
        mesh=mesh,
        in_specs=(P(None, None, "wn", "sp"), P(None, "wn"), P("wn")),
        out_specs=P(None, None, "wn", "sp"),
        check_vma=False,
    )
```

```python
import functools

import jax
import jax.numpy as jnp
import numpy as np
from jax import lax
from jax.experimental import pallas as pl
from jax.experimental.pallas import tpu as pltpu
from jax.sharding import PartitionSpec as P


H = 64
T = 128
EPS = 1e-06
NB = 15
NA = 24 - NB
F32 = jnp.float32
BF = jnp.bfloat16


def band():
    k = np.arange(-H, H + 1, dtype=np.float64)
    norm = np.sqrt(np.sum(np.exp(-np.pi * k * k / (H / 2.0) ** 2)))
    src = np.concatenate([np.arange(T), np.arange(-H, 0), np.arange(T, T + H)])
    lag = src[:, None] - np.arange(T)[None, :]
    val = np.exp(-np.pi * lag * lag / (2.0 * (H / 2.0) ** 2)) / norm
    return np.where(np.abs(lag) <= H, val, 0.0).astype(np.float32)


def pieces(v):
    h = v.astype(BF)
    r = v - h.astype(F32)
    m = r.astype(BF)
    return h, m, (r - m.astype(F32)).astype(BF)


def bands():
    b = band()
    h = b.astype(BF)
    m = (b - h.astype(np.float32)).astype(BF)
    low = (b - h.astype(np.float32) - m.astype(np.float32)).astype(BF)
    across = np.concatenate([h, m, low], axis=1)
    return np.ascontiguousarray(across), np.ascontiguousarray(across.T)


def parity(axis):
    return lax.axis_index(axis) % 2


def lanes_low(shape):
    return lax.broadcasted_iota(jnp.int32, shape, len(shape) - 1) < H


def half_turn(v):
    return pltpu.roll(v, H, 1)


def edges(v, even):
    low = lanes_low((H, T))
    a, b = v[:H], v[H:]
    right = jnp.where(low, half_turn(a), b)
    left = jnp.where(low, a, half_turn(b))
    return jnp.where(even, right, left), jnp.where(even, left, right)


def joined(re, ro, even):
    low = lanes_low((H, T))
    hl = jnp.where(even, ro, re)
    hr = jnp.where(even, re, ro)
    return jnp.concatenate(
        [jnp.where(low, hl, half_turn(hr)), jnp.where(low, half_turn(hl), hr)], axis=0
    )


def mm(a, b):
    return jnp.dot(a, b, preferred_element_type=F32)


def y_pass(bt, x, re, ro, even):
    cols = []
    for v, e, o in zip(x, re, ro):
        up = jnp.where(even, o, e)
        down = jnp.where(even, e, o)
        cols.append(jnp.concatenate([v, up, down], axis=0))
    w = cols[0] if len(cols) == 1 else jnp.concatenate(cols, axis=1)
    h, m, low = pieces(w)
    p = mm(bt, h)
    q = mm(bt[: 2 * T], m)
    r = mm(bt[:T], low)
    out = p[:T] + ((p[T : 2 * T] + q[:T]) + (p[2 * T :] + (q[T:] + r)))
    return [out[:, T * i : T * (i + 1)] for i in range(len(cols))]


def z_pass(b, x, re, ro, even):
    rows = [
        jnp.concatenate([v, joined(e, o, even)], axis=1) for v, e, o in zip(x, re, ro)
    ]
    w = rows[0] if len(rows) == 1 else jnp.concatenate(rows, axis=0)
    h, m, low = pieces(w)
    p = mm(h, b)
    q = mm(m, b[:, : 2 * T])
    r = mm(low, b[:, :T])
    out = p[:, :T] + (
        (p[:, T : 2 * T] + q[:, :T]) + (p[:, 2 * T :] + (q[:, T:] + r))
    )
    return [out[T * i : T * (i + 1)] for i in range(len(rows))]


def cuts(n, step):
    return [range(i, min(i + step, n)) for i in range(0, n, step)]


def pack_y_kernel(src, yo, sem):
    off = pl.multiple_of(parity("wn") * H, H)
    copy = pltpu.make_async_copy(src.at[pl.ds(0, NB), pl.ds(off, H)], yo, sem.at[0])
    copy.start()
    copy.wait()


def pack_z_kernel(x, zo, ze, ye):
    zeven, yeven = parity("sp") == 0, parity("wn") == 0
    for p in range(NA):
        e, o = edges(x[NB + p], zeven)
        ze[p] = e
        zo[p] = o
    for p in range(NB):
        ye[p] = jnp.where(yeven, x[p, H:], x[p, :H])


def y_first_kernel(bt, x, ro, re, n, zo, ze):
    zeven, yeven = parity("sp") == 0, parity("wn") == 0
    for c in cuts(NB, 2):
        got = y_pass(bt[...], [x[p] for p in c], [re[p] for p in c], [ro[p] for p in c], yeven)
        for p, v in zip(c, got):
            n[p] = v
            e, o = edges(v, zeven)
            ze[p] = e
            zo[p] = o


def z_first_kernel(b, x, ro, re, n, yo, ye):
    zeven, yeven = parity("sp") == 0, parity("wn") == 0
    for c in cuts(NA, 3):
        got = z_pass(
            b[...], [x[NB + p] for p in c], [re[p] for p in c], [ro[p] for p in c], zeven
        )
        for p, v in zip(c, got):
            n[p] = v
            yo[p] = jnp.where(yeven, v[:H], v[H:])
            ye[p] = jnp.where(yeven, v[H:], v[:H])


def put_stats(acc, f, p):
    lane = lax.broadcasted_iota(jnp.int32, (T, T), 1)
    mean = jnp.sum(f, axis=1, keepdims=True) * (1.0 / T)
    c = f - mean
    second = jnp.sum(c * c, axis=1, keepdims=True)
    acc = jnp.where(lane == p, mean, acc)
    return jnp.where(lane == p + 24, second, acc)


def last(one_pass, step, axis, base, first, *refs):
    b, x, ro, re = refs[:4]
    f, st = refs[-2:]
    even = parity(axis) == 0
    acc = jnp.zeros((T, T), F32) if first else refs[4][...]
    for c in cuts(f.shape[0], step):
        got = one_pass(b[...], [x[p] for p in c], [re[p] for p in c], [ro[p] for p in c], even)
        for p, v in zip(c, got):
            f[p] = v
            acc = put_stats(acc, v, base + p)
    if first:
        st[...] = acc
    else:
        flat = acc.T[:48]
        for q in range(st.shape[0]):
            st[q] = flat


def merge(st, tiles):
    n = st.shape[0]
    parts = [st[q] for q in range(n)]
    mean = sum(q[:24] for q in parts) * (1.0 / n)
    second = sum(q[24:] for q in parts)
    spread = sum((q[:24] - mean) * (q[:24] - mean) for q in parts)
    return mean, second + spread * float(tiles * T)


def mid_kernel(st, out):
    mean, second = merge(st, 1)
    for q in range(out.shape[0]):
        out[q, :24] = mean
        out[q, 24:] = second


def factor_kernel(stress, profile, wide):
    s = stress[...]
    a11 = jnp.sqrt(s[0:1])
    a21 = s[3:4] / a11
    a22 = jnp.sqrt(s[1:2] - a21 * a21)
    a31 = s[4:5] / a11
    a32 = (s[5:6] - a21 * a31) / a22
    a33 = jnp.sqrt(s[2:3] - a31 * a31 - a32 * a32)
    rows = [a11, a21, a22, a31, a32, a33, profile[...].reshape(1, T), a11]
    cols = jnp.concatenate(rows + [jnp.zeros((T - 8, T), F32)], axis=0).T
    for q in range(7):
        wide[q] = jnp.broadcast_to(cols[:, q : q + 1], (T, T))


def final_kernel(fb, fa, st, wide, out, buf, sems):
    mean, second = merge(st, 8)
    inv = 1.0 / jnp.sqrt(second * (1.0 / 4096.0) + EPS)
    cols = jnp.concatenate([mean, inv, jnp.zeros((T - 48, T), F32)], axis=0).T
    copies = []
    for k in range(8):
        g = []
        for c in range(3):
            p = 3 * k + c
            v = fb[p] if p < NB else fa[p - NB]
            g.append((v - cols[:, p : p + 1]) * cols[:, 24 + p : 25 + p])
        buf[k, 0] = wide[6] + wide[0] * g[0]
        buf[k, 1] = wide[1] * g[0] + wide[2] * g[1]
        buf[k, 2] = wide[3] * g[0] + wide[4] * g[1] + wide[5] * g[2]
        copy = pltpu.make_async_copy(buf.at[k], out.at[k], sems.at[k])
        copy.start()
        copies.append(copy)
    for copy in copies:
        copy.wait()


def call(kernel, ins, outs, scratch=(), hbm_out=False, hbm_in=()):
    vmem = pl.BlockSpec(memory_space=pltpu.VMEM)
    args, specs = [], []
    for i, a in enumerate(ins):
        if i in hbm_in:
            args.append(pltpu.with_memory_space_constraint(a, pltpu.HBM))
            specs.append(pl.BlockSpec(memory_space=pl.ANY))
        else:
            args.append(pltpu.with_memory_space_constraint(a, pltpu.VMEM))
            specs.append(vmem)
    if hbm_out:
        shapes = [jax.ShapeDtypeStruct(s, F32) for s in outs]
        out_specs = [pl.BlockSpec(memory_space=pl.ANY) for s in outs]
    else:
        shapes = [pltpu.VMEM(s, F32) for s in outs]
        out_specs = [vmem for s in outs]
    return pl.pallas_call(
        kernel,
        in_specs=specs,
        out_specs=out_specs,
        out_shape=shapes,
        scratch_shapes=list(scratch),
        compiler_params=pltpu.CompilerParams(vmem_limit_bytes=24 << 20),
    )(*args)


def swap(v, axis, odd, periodic):
    n = lax.axis_size(axis)
    pairs = []
    for i in range(odd, n, 2):
        j = (i + 1) % n
        if periodic or j > i:
            pairs += [(i, j), (j, i)]
    return lax.ppermute(v, axis, pairs)


def groups(nx, nz):
    zs = [[x * nz + z for z in range(nz)] for x in range(nx)]
    xs = [[x * nz + z for x in range(nx)] for z in range(nz)]
    return zs, xs


def run(random_slabs, stress, profile):
    x = random_slabs.reshape(24, T, T)
    b, bt = (jnp.asarray(v) for v in bands())
    hb, ha = (NB, H, T), (NA, H, T)
    fb, fa = (NB, T, T), (NA, T, T)
    (yo,) = call(
        pack_y_kernel, [x], [hb], scratch=[pltpu.SemaphoreType.DMA((1,))], hbm_in=(0,)
    )
    yo = swap(yo, "wn", 1, False)
    zo, ze, ye = call(pack_z_kernel, [x], [ha, ha, hb])
    zo = swap(zo, "sp", 1, True)
    ye = swap(ye, "wn", 0, False)
    ze = swap(ze, "sp", 0, True)
    n_b, zo_b, ze_b = call(y_first_kernel, [bt, x, yo, ye], [fb, hb, hb])
    zo_b = swap(zo_b, "sp", 1, True)
    ze_b = swap(ze_b, "sp", 0, True)
    n_a, yo_a, ye_a = call(z_first_kernel, [b, x, zo, ze], [fa, ha, ha])
    yo_a = swap(yo_a, "wn", 1, False)
    ye_a = swap(ye_a, "wn", 0, False)
    (wide,) = call(factor_kernel, [stress, profile], [(7, T, T)])
    f_a, s_a = call(
        functools.partial(last, y_pass, 2, "wn", NB, True),
        [bt, n_a, yo_a, ye_a],
        [fa, (T, T)],
    )
    f_b, st = call(
        functools.partial(last, z_pass, 3, "sp", 0, False),
        [b, n_b, zo_b, ze_b, s_a],
        [fb, (8, 48, T)],
    )
    zs, xs = groups(4, 8)
    st = lax.all_to_all(st, "sp", 0, 0, axis_index_groups=zs, tiled=True)
    (st,) = call(mid_kernel, [st], [(4, 48, T)])
    st = lax.all_to_all(st, "sp", 0, 0, axis_index_groups=xs, tiled=True)
    (out,) = call(
        final_kernel,
        [f_b, f_a, st, wide],
        [(8, 3, T, T)],
        scratch=[pltpu.VMEM((8, 3, T, T), F32), pltpu.SemaphoreType.DMA((8,))],
        hbm_out=True,
    )
    return out


def solution(mesh):
    return jax.shard_map(
        run,
        mesh=mesh,
        in_specs=(P(None, None, "wn", "sp"), P(None, "wn"), P("wn")),
        out_specs=P(None, None, "wn", "sp"),
        check_vma=False,
    )
```
